32 devices in a mesh: tm: 8 (over z, x), space: 4 (over y, core).
Axes of the slice: x: 2, y: 2, z: 4, core: 2. Of those that a mesh axis runs over, the one named last changes fastest.
Arguments:
- checkpoint: float32 [8, 4, 64, 1024], P('tm', None, 'space'), may hold values from -6 to 6
- advect: float32 [8, 2, 64, 1024], P('tm', None, 'space'), may hold values from -0.2 to 0.2
- diffuse: float32 [8, 64, 1024], P('tm', 'space'), may hold values from 0.1 to 0.2
- obs_rows: int32 [8, 8, 8], P('tm', None, 'space'), may hold values from 0 to 1
- obs_values: float32 [8, 8, 8, 4, 8, 1024], P('tm', None, 'space'), may hold values from -6 to 6
- obs_weight: float32 [8], P('tm'), may hold values from 0.5 to 13.5
- error_inverse: float32 [8, 4], P('tm'), may hold values from 0.3 to 3
- rates: float32 [8, 4], replicated, may hold values from 0.07924466 to 1, as said below
Outputs:
- direction: float32 [8, 4, 64, 1024], P('tm', None, 'space')
- grad_rms: float32 [], replicated
The draws below stay inside these ranges and needn't reach their ends.
Inputs may be any that keep to these rules, and one draw needn't show every extreme that they name: `obs_rows`: entry i of the last dimension counts blocks of 8 rows within the rows of space block i // 2; repeats may occur. `rates`: every entry is below 1.
All inputs are finite; a program needn't handle non-finite values.
Results may differ from the reference program's by a relative error of at most 0.0003.
Values sent between devices are 32-bit elements; how exact they have to be, the bound alone decides.
A program may use at most 64 MiB of HBM per device.

```python
import math
import jax
import jax.numpy as jnp
from jax import lax

STATE_COMPONENTS = 4
NX = 1024
ROWS = 16
STEPS = 8
BLOCK = 8
KOBS = 2
SUBWINDOW_COUNT = 8
NY = 64
NOBS = 8


def draw_obs_weight(key, part):
    places = jnp.arange(SUBWINDOW_COUNT, dtype=jnp.float32) / max(SUBWINDOW_COUNT - 1, 1)
    rising = 3.0 ** places
    jitter = jax.random.uniform(key, (SUBWINDOW_COUNT,), jnp.float32, 0.8, 1.2)
    return rising * jitter


def draw_rates(key, part):
    random_key_parts = jax.random.split(jax.random.fold_in(key, 7), 5)
    slow_share = 0.5
    is_slow = jax.random.uniform(random_key_parts[0], (STATE_COMPONENTS,), jnp.float32) < slow_share
    slow_strength = jax.random.uniform(random_key_parts[1], (STATE_COMPONENTS,), jnp.float32, 0.15, 0.4)
    fast_strength = jax.random.uniform(random_key_parts[1], (STATE_COMPONENTS,), jnp.float32, 2.0, 4.0)
    strength = jnp.where(is_slow, slow_strength, fast_strength)
    factor = jnp.exp(jax.random.uniform(random_key_parts[2], (SUBWINDOW_COUNT, STATE_COMPONENTS), jnp.float32, jnp.log(0.6), jnp.log(1.6)))
    logarithm_rate = jnp.log(0.1) * strength[None, :] * factor / SUBWINDOW_COUNT
    surge_location = jax.random.randint(random_key_parts[3], (2, STATE_COMPONENTS), 0, SUBWINDOW_COUNT)
    inside_surge = jnp.any(jnp.arange(SUBWINDOW_COUNT)[:, None, None] == surge_location[None, :, :], axis=1)
    reduction_factor = jax.random.uniform(random_key_parts[4], (SUBWINDOW_COUNT, STATE_COMPONENTS), jnp.float32, 0.5, 0.8)
    return jnp.exp(logarithm_rate) * jnp.where(inside_surge, reduction_factor, 1.0)


def with_ends(entries, stream_key, smallest, largest):
    longest = entries.shape.index(max(entries.shape))
    spots = []
    for shift in (0, 1):
        where = [jax.random.randint(jax.random.fold_in(stream_key, axis), (), 0, length) for axis, length in enumerate(entries.shape)]
        where[longest] = (where[longest] + shift) % entries.shape[longest]
        spots.append(tuple(where))
    return entries.at[spots[0]].set(smallest).at[spots[1]].set(largest)


def steps_of(key, shape, cuts, smallest, largest):
    gain = 1.0
    for position, parts in cuts:
        heights = jax.random.uniform(jax.random.fold_in(jax.random.fold_in(key, 6), position), (parts,), jnp.float32, smallest / len(cuts), largest / len(cuts))
        gain = gain * jnp.repeat(jnp.exp(heights), shape[position] // parts).reshape((-1,) + (1,) * (len(shape) - 1 - position))
    return gain


def gaussian(stream_key, dims, deviation, limit, cuts=(), held_as=jnp.bfloat16):
    drawn = jax.random.normal(stream_key, dims, jnp.float32) * deviation
    if len(cuts) > 0:
        drawn = steps_of(stream_key, dims, cuts, -0.22, 0.18) * drawn
    return jnp.clip(drawn, min=-limit, max=limit).astype(held_as)


def setup_inputs(seed: int = 0) -> dict:
    keys = jax.random.split(jax.random.key(seed), 9)
    checkpoint = gaussian(keys[0], (SUBWINDOW_COUNT, STATE_COMPONENTS, NY, NX), 1.0, 6.0, ((0, 8), (2, 4)), jnp.float32)
    advect = jnp.clip(jax.random.uniform(keys[1], (SUBWINDOW_COUNT, 2, NY, NX), jnp.float32, -0.2, 0.2) * steps_of(keys[1], (SUBWINDOW_COUNT, 2, NY, NX), ((0, 8), (2, 4)), -0.4, 0.0), -0.2, 0.2)
    diffuse = jnp.clip(0.1 + 0.1 * jax.random.uniform(keys[2], (SUBWINDOW_COUNT, NY, NX), jnp.float32) ** steps_of(keys[2], (SUBWINDOW_COUNT, NY, NX), ((0, 8), (1, 4)), -0.2, 0.2), 0.1, 0.2)
    obs_rows = with_ends(jax.random.randint(keys[3], (SUBWINDOW_COUNT, STEPS, NOBS), 0, ROWS // BLOCK), jax.random.fold_in(keys[3], 1), 0, (ROWS // BLOCK) - 1).astype(jnp.int32)
    obs_values = gaussian(keys[4], (SUBWINDOW_COUNT, STEPS, NOBS, STATE_COMPONENTS, BLOCK, NX), 1.0, 6.0, ((0, 8), (2, 4)), jnp.float32)
    obs_weight = draw_obs_weight(jax.random.fold_in(keys[8], 71), 0)
    error_inverse = jnp.clip(jnp.exp(math.log(3.0) - 2.3025851 * jax.random.uniform(keys[6], (SUBWINDOW_COUNT, STATE_COMPONENTS), jnp.float32) ** steps_of(keys[6], (SUBWINDOW_COUNT, STATE_COMPONENTS), ((0, 8),), -0.2, 0.2)), 0.3, 3.0)
    rates = draw_rates(jax.random.fold_in(keys[8], 71), 0)
    return {"checkpoint": checkpoint, "advect": advect, "diffuse": diffuse, "obs_rows": obs_rows, "obs_values": obs_values, "obs_weight": obs_weight, "error_inverse": error_inverse, "rates": rates}


def weights_of(advect_one, diffuse_one):
    centre = 1.0 - 4.0 * diffuse_one
    to_east = diffuse_one - 0.5 * advect_one[0]
    to_west = diffuse_one + 0.5 * advect_one[0]
    to_north = diffuse_one - 0.5 * advect_one[1]
    to_south = diffuse_one + 0.5 * advect_one[1]
    return (centre, to_east, to_west, to_north, to_south)

def pad_rows(values_in):
    return jnp.pad(values_in, ((0, 0), (1, 1), (0, 0)))

def advance(field_now, stencil):
    centre, to_east, to_west, to_north, to_south = stencil
    padded = pad_rows(field_now)
    return centre * field_now + to_east * jnp.roll(field_now, -1, axis=2) + to_west * jnp.roll(field_now, 1, axis=2) + to_north * padded[:, 2:] + to_south * padded[:, :-2]

def retreat(costate, stencil):
    centre, to_east, to_west, to_north, to_south = stencil
    north_flux = pad_rows(to_north * costate)
    south_flux = pad_rows(to_south * costate)
    return centre * costate + jnp.roll(to_east * costate, 1, axis=2) + jnp.roll(to_west * costate, -1, axis=2) + north_flux[:, :-2] + south_flux[:, 2:]

def row_index(rows_step):
    first_rows = jnp.arange(NOBS, dtype=jnp.int32) // KOBS * ROWS + rows_step.astype(jnp.int32) * BLOCK
    return first_rows[:, None] + jnp.arange(BLOCK, dtype=jnp.int32)[None, :]

def observe(field_now, row_picks):
    return jnp.transpose(field_now[:, row_picks], (1, 0, 2, 3))

def spread(misfit, row_picks):
    empty_field = jnp.zeros((STATE_COMPONENTS, NY, NX), jnp.float32)
    return empty_field.at[:, row_picks].add(jnp.transpose(misfit, (1, 0, 2, 3)))

def sweep_forward(packed):
    initial, advect_one, diffuse_one, rows_one, values_one = packed
    stencil = weights_of(advect_one, diffuse_one)
    field_now = initial
    misfits = []
    for moment in range(STEPS):
        field_now = advance(field_now, stencil)
        misfits.append(observe(field_now, row_index(rows_one[moment])) - values_one[moment])
    return (field_now, jnp.stack(misfits))

def sweep_back(packed):
    advect_one, diffuse_one, rows_one, misfit_one, obs_scale, next_term, own_term = packed
    stencil = weights_of(advect_one, diffuse_one)
    costate = spread(obs_scale * misfit_one[STEPS - 1], row_index(rows_one[STEPS - 1])) - next_term
    for moment in range(STEPS, 0, -1):
        costate = retreat(costate, stencil)
        if moment >= 2:
            costate = costate + spread(obs_scale * misfit_one[moment - 2], row_index(rows_one[moment - 2]))
    return costate + own_term

def forward_carry(running, packed):
    rate_row, inno_row, grad_one = packed
    updated = rate_row[:, None, None] * running + inno_row[:, None, None] * grad_one
    return (updated, updated)

def backward_carry(running, packed):
    rate_row, inno_row, forward_one = packed
    updated = inno_row[:, None, None] * forward_one + rate_row[:, None, None] * running
    return (updated, updated)

def reference(checkpoint, advect, diffuse, obs_rows, obs_values, obs_weight, error_inverse, rates):
    end_states, misfits = lax.map(sweep_forward, (checkpoint, advect, diffuse, obs_rows, obs_values))
    prior_end = jnp.concatenate([jnp.zeros_like(end_states[:1]), end_states[:-1]], axis=0)
    forcing = checkpoint - prior_end
    weighted = error_inverse[:, :, None, None] * forcing
    next_term = jnp.concatenate([weighted[1:], jnp.zeros_like(weighted[:1])], axis=0)
    gradient = lax.map(sweep_back, (advect, diffuse, obs_rows, misfits, obs_weight, next_term, weighted))
    square_sum = jnp.sum(gradient * gradient)
    rms_value = jnp.sqrt(square_sum / (SUBWINDOW_COUNT * STATE_COMPONENTS * NY * NX) + 1e-06)
    innovation = jnp.sqrt(1.0 - rates * rates)
    next_rates = jnp.concatenate([rates[1:], jnp.zeros((1, STATE_COMPONENTS), jnp.float32)], axis=0)
    zero_field = jnp.zeros((STATE_COMPONENTS, NY, NX), jnp.float32)
    _, smoothed = lax.scan(forward_carry, zero_field, (rates, innovation, gradient))
    _, result = lax.scan(backward_carry, zero_field, (next_rates, innovation, smoothed), reverse=True)
    return (result / rms_value, rms_value)
```

```python
import functools

import jax
import jax.numpy as jnp
from jax import lax
from jax.experimental import pallas as pl
from jax.experimental.pallas import tpu as pltpu
from jax.sharding import PartitionSpec as P

MESH = pl.DeviceIdType.MESH
LANES = 128


def kernel(
    tm,
    space,
    rows_smem,
    weight_smem,
    einv_smem,
    rates_smem,
    ck_hbm,
    adv_hbm,
    dif_hbm,
    obs_hbm,
    back_ref,
    sums_ref,
    states,
    adv,
    dif,
    coef,
    obs,
    pull,
    count,
    next_ck,
    next_einv,
    prior_end,
    costate,
    grads,
    gathered,
    scanned,
    part,
    part_tm,
    part_space,
    local_sem,
    halo_send,
    halo_recv,
    pull_send,
    pull_recv,
    edge_send,
    edge_recv,
    a2a_send,
    a2a_recv,
    ret_send,
    ret_recv,
    sum_send,
    sum_recv,
):
    comps, rows, cols = ck_hbm.shape
    steps, kobs, _, block, _ = obs_hbm.shape
    halo = 2 * steps
    wide = rows + 2 * halo
    share = grads.shape[1]
    tiles = rows // block
    me = lax.axis_index("tm")
    sp = lax.axis_index("space")
    own = pl.ds(halo, rows)
    copies = []

    def send(src, dst, ssem, rsem, target, guard=None):
        copy = pltpu.make_async_remote_copy(
            src_ref=src, dst_ref=dst, send_sem=ssem, recv_sem=rsem,
            device_id=target, device_id_type=MESH,
        )
        if guard is None:
            copy.start()
        else:
            pl.when(guard)(copy.start)
        copies.append((copy, guard))
        return copy

    def landed(copy, guard=None):
        if guard is None:
            copy.wait_recv()
        else:
            pl.when(guard)(copy.wait_recv)

    has_north = sp < space - 1
    has_south = sp > 0
    north = {"space": jnp.minimum(sp + 1, space - 1)}
    south = {"space": jnp.maximum(sp - 1, 0)}
    has_next = me < tm - 1
    has_prev = me > 0
    nxt = {"tm": jnp.minimum(me + 1, tm - 1)}
    prv = {"tm": jnp.maximum(me - 1, 0)}

    loads = [
        pltpu.make_async_copy(dif_hbm, dif.at[own], local_sem.at[0]),
        pltpu.make_async_copy(adv_hbm, adv.at[:, own], local_sem.at[1]),
        pltpu.make_async_copy(ck_hbm, states.at[0, :, own], local_sem.at[2]),
        pltpu.make_async_copy(obs_hbm, obs, local_sem.at[3]),
    ]
    for load in loads:
        load.start()

    barrier = pltpu.get_barrier_semaphore()
    for o in range(1, tm):
        pl.semaphore_signal(
            barrier, inc=1, device_id={"tm": lax.rem(me + o, tm)}, device_id_type=MESH
        )
    for o in range(1, space):
        pl.semaphore_signal(
            barrier, inc=1, device_id={"space": lax.rem(sp + o, space)}, device_id_type=MESH
        )

    weight = weight_smem[0]
    low_halo = pl.ds(0, halo)
    high_halo = pl.ds(halo + rows, halo)

    @pl.when(jnp.logical_not(has_south))
    def _():
        states[0, :, 0:halo, :] = jnp.zeros((comps, halo, cols), jnp.float32)
        adv[:, 0:halo, :] = jnp.zeros((2, halo, cols), jnp.float32)
        dif[0:halo, :] = jnp.zeros((halo, cols), jnp.float32)
        pull[:, :, 0:block, :] = jnp.zeros((steps, comps, block, cols), jnp.float32)
        count[:, 0] = jnp.zeros((steps, block, LANES), jnp.float32)

    @pl.when(jnp.logical_not(has_north))
    def _():
        states[0, :, halo + rows : wide, :] = jnp.zeros((comps, halo, cols), jnp.float32)
        adv[:, halo + rows : wide, :] = jnp.zeros((2, halo, cols), jnp.float32)
        dif[halo + rows : wide, :] = jnp.zeros((halo, cols), jnp.float32)
        pull[:, :, block + rows :, :] = jnp.zeros((steps, comps, block, cols), jnp.float32)
        count[:, tiles + 1] = jnp.zeros((steps, block, LANES), jnp.float32)

    @pl.when(jnp.logical_not(has_next))
    def _():
        next_ck[...] = jnp.zeros_like(next_ck)
        next_einv[...] = jnp.zeros_like(next_einv)

    @pl.when(jnp.logical_not(has_prev))
    def _():
        prior_end[...] = jnp.zeros_like(prior_end)

    for c in range(comps):
        part[1, c : c + 1, :] = jnp.full((1, LANES), einv_smem[0, c], jnp.float32)

    @pl.loop(0, steps)
    def _(t):
        for b in range(tiles):
            total = jnp.float32(0.0)
            for i in range(kobs):
                total = total + jnp.where(rows_smem[t, i] == b, weight, 0.0)
            count[t, b + 1] = jnp.full((block, LANES), total, jnp.float32)

    for load in loads[:3]:
        load.wait()
    pl.semaphore_wait(barrier, tm + space - 2)

    halos = []
    for k, (ref, sem) in enumerate(((dif, 0), (adv, 1), (states.at[0], 2))):
        lead = (slice(None),) * (len(ref.shape) - 2)
        source = ref.at[lead + (own,)]
        halos.append(
            (
                send(source, ref.at[lead + (low_halo,)], halo_send.at[0, k], halo_recv.at[0, k], north, has_north),
                send(source, ref.at[lead + (high_halo,)], halo_send.at[1, k], halo_recv.at[1, k], south, has_south),
            )
        )
    ck_copy = send(states.at[0, :, own], next_ck, edge_send.at[0], edge_recv.at[0], prv, has_prev)
    einv_copy = send(part.at[1], next_einv, edge_send.at[1], edge_recv.at[1], prv, has_prev)
    count_copies = (
        send(count.at[:, tiles], count.at[:, 0], halo_send.at[0, 3], halo_recv.at[0, 3], north, has_north),
        send(count.at[:, 1], count.at[:, tiles + 1], halo_send.at[1, 3], halo_recv.at[1, 3], south, has_south),
    )

    loads[3].wait()

    @pl.loop(0, steps)
    def _(t):
        for b in range(tiles):
            picks = [jnp.where(rows_smem[t, i] == b, weight, 0.0) for i in range(kobs)]
            for c in range(comps):
                total = picks[0] * obs[t, 0, c]
                for i in range(1, kobs):
                    total = total + picks[i] * obs[t, i, c]
                pull[t, c, block * (b + 1) : block * (b + 2), :] = total

    pull_copies = {}

    def send_pull(t):
        pull_copies[t] = (
            send(
                pull.at[t, :, pl.ds(rows, block)], pull.at[t, :, pl.ds(0, block)],
                pull_send.at[0, t], pull_recv.at[0, t], north, has_north,
            ),
            send(
                pull.at[t, :, pl.ds(block, block)], pull.at[t, :, pl.ds(block + rows, block)],
                pull_send.at[1, t], pull_recv.at[1, t], south, has_south,
            ),
        )

    for t in range(steps - 2, -1, -1):
        send_pull(t)

    def both_landed(pair):
        landed(pair[0], has_south)
        landed(pair[1], has_north)

    both_landed(halos[0])
    both_landed(halos[1])
    for r in range(0, wide, 8):
        at = slice(r, r + 8)
        d, a0, a1 = dif[at], adv[0, at], adv[1, at]
        coef[0, at] = 1.0 - 4.0 * d
        coef[1, at] = d - 0.5 * a0
        coef[2, at] = d + 0.5 * a0
        coef[3, at] = d - 0.5 * a1
        coef[4, at] = d + 0.5 * a1
    both_landed(halos[2])

    def forward(c):
        @pl.loop(0, steps)
        def _(t):
            v = states[t, c]
            states[t + 1, c] = (
                coef[0] * v
                + coef[1] * pltpu.roll(v, cols - 1, 1)
                + coef[2] * pltpu.roll(v, 1, 1)
                + coef[3] * pltpu.roll(v, wide - 1, 0)
                + coef[4] * pltpu.roll(v, 1, 0)
            )

    half = comps // 2

    @pl.loop(0, half)
    def _(c):
        forward(c)

    landed(ck_copy, has_next)
    landed(einv_copy, has_next)

    @pl.loop(0, comps)
    def _(c):
        scale = jnp.concatenate([next_einv[pl.ds(c, 1), :]] * (cols // LANES), axis=1)
        inner = pl.ds(block, rows)
        pull[steps - 1, c, inner] = pull[steps - 1, c, inner] + scale * next_ck[c]

    send_pull(steps - 1)

    @pl.loop(half, comps)
    def _(c):
        forward(c)

    end_copy = send(
        states.at[steps, :, own], prior_end, edge_send.at[2], edge_recv.at[2], nxt, has_next
    )

    both_landed(count_copies)
    for t in range(steps - 1, -1, -1):
        both_landed(pull_copies[t])

    inner_rows = rows + 2 * block
    first = halo - block
    inner = pl.ds(first, inner_rows)

    def adjoint(c):
        scale = jnp.concatenate([next_einv[pl.ds(c, 1), :]] * (cols // LANES), axis=1)

        def force(t):
            marks = [
                jnp.concatenate([count[t, q]] * (cols // LANES), axis=1) for q in range(tiles + 2)
            ]
            return jnp.concatenate(marks, axis=0) * states[t + 1, c, inner] - pull[t, c]

        costate[...] = force(steps - 1) + scale * states[steps, c, inner]

        def step(w):
            return (
                coef[0, inner] * w
                + pltpu.roll(coef[1, inner] * w, 1, 1)
                + pltpu.roll(coef[2, inner] * w, cols - 1, 1)
                + pltpu.roll(coef[3, inner] * w, 1, 0)
                + pltpu.roll(coef[4, inner] * w, inner_rows - 1, 0)
            )

        @pl.loop(0, steps - 1)
        def _(s):
            costate[...] = step(costate[...]) + force(steps - 2 - s)

        last = step(costate[...])[block : block + rows]
        states[0, c, 0:rows, :] = last

    @pl.loop(0, comps)
    def _(c):
        adjoint(c)

    landed(end_copy, has_prev)

    per = rows // share
    squares = jnp.zeros((8, LANES), jnp.float32)
    for c in range(comps):
        scale = einv_smem[0, c]
        g = states[0, c, 0:rows, :] + scale * (states[0, c, own] - prior_end[c])
        for h in range(per):
            grads[c * per + h] = g[h * share : (h + 1) * share]
        sq = g * g
        for r in range(0, rows, 8):
            for l in range(0, cols, LANES):
                squares = squares + sq[r : r + 8, l : l + LANES]
    part[0] = squares

    gather = []
    sums = []
    for o in range(1, tm):
        peer = lax.rem(me + o, tm)
        gather.append(
            send(grads.at[peer], gathered.at[me], a2a_send.at[o], a2a_recv.at[o], {"tm": peer})
        )
    for o in range(1, tm):
        peer = lax.rem(me + o, tm)
        sums.append(
            send(part.at[0], part_tm.at[me], sum_send.at[o], sum_recv.at[o], {"tm": peer})
        )
    part_tm[me] = squares
    gathered[me] = grads[me]
    for copy in gather:
        copy.wait_recv()

    k = me * share // rows

    def rate(j):
        return jnp.full((1, cols), rates_smem[j, k], jnp.float32)

    running = jnp.zeros((share, cols), jnp.float32)
    for j in range(tm):
        r = rate(j)
        running = r * running + jnp.sqrt(1.0 - r * r) * gathered[j]
        scanned[j] = running
    running = jnp.zeros((share, cols), jnp.float32)
    for j in range(tm - 1, -1, -1):
        r = rate(j)
        running = jnp.sqrt(1.0 - r * r) * scanned[j] + running
        scanned[j] = running
        running = r * running

    returns = []
    for o in range(1, tm):
        peer = lax.rem(me + o, tm)
        returns.append(
            send(scanned.at[peer], back_ref.at[me], ret_send.at[o], ret_recv.at[o], {"tm": peer})
        )
    back_ref[me] = scanned[me]

    for copy in sums:
        copy.wait_recv()
    total = part_tm[0]
    for j in range(1, tm):
        total = total + part_tm[j]
    part_space[sp] = total
    part[2] = total
    across = []
    for o in range(1, space):
        peer = lax.rem(sp + o, space)
        across.append(
            send(part.at[2], part_space.at[sp], sum_send.at[tm + o], sum_recv.at[tm + o], {"space": peer})
        )
    for copy in across:
        copy.wait_recv()
    total = part_space[0]
    for j in range(1, space):
        total = total + part_space[j]
    sums_ref[...] = total
    for copy in returns:
        copy.wait_recv()
    for copy, guard in copies:
        if guard is None:
            copy.wait_send()
        else:
            pl.when(guard)(copy.wait_send)


def on_device(tm, space, checkpoint, advect, diffuse, obs_rows, obs_values, obs_weight, error_inverse, rates):
    comps, rows, cols = checkpoint.shape[1:]
    steps, kobs, _, block, _ = obs_values.shape[1:]
    halo = 2 * steps
    wide = rows + 2 * halo
    tiles = rows // block
    share = comps * rows // tm
    f32 = jnp.float32
    smem = pl.BlockSpec(memory_space=pltpu.SMEM)
    hbm = pl.BlockSpec(memory_space=pl.ANY)
    vmem = pl.BlockSpec(memory_space=pltpu.VMEM)
    dma = pltpu.SemaphoreType.DMA
    back, sums = pl.pallas_call(
        functools.partial(kernel, tm, space),
        out_shape=(
            jax.ShapeDtypeStruct((tm, share, cols), f32),
            jax.ShapeDtypeStruct((8, LANES), f32),
        ),
        in_specs=[smem] * 4 + [hbm] * 4,
        out_specs=(vmem, vmem),
        scratch_shapes=[
            pltpu.VMEM((steps + 1, comps, wide, cols), f32),
            pltpu.VMEM((2, wide, cols), f32),
            pltpu.VMEM((wide, cols), f32),
            pltpu.VMEM((5, wide, cols), f32),
            pltpu.VMEM((steps, kobs, comps, block, cols), f32),
            pltpu.VMEM((steps, comps, rows + 2 * block, cols), f32),
            pltpu.VMEM((steps, tiles + 2, block, LANES), f32),
            pltpu.VMEM((comps, rows, cols), f32),
            pltpu.VMEM((8, LANES), f32),
            pltpu.VMEM((comps, rows, cols), f32),
            pltpu.VMEM((rows + 2 * block, cols), f32),
            pltpu.VMEM((tm, share, cols), f32),
            pltpu.VMEM((tm, share, cols), f32),
            pltpu.VMEM((tm, share, cols), f32),
            pltpu.VMEM((3, 8, LANES), f32),
            pltpu.VMEM((tm, 8, LANES), f32),
            pltpu.VMEM((space, 8, LANES), f32),
            dma((4,)),
            dma((2, 4)),
            dma((2, 4)),
            dma((2, steps)),
            dma((2, steps)),
            dma((3,)),
            dma((3,)),
            dma((tm,)),
            dma((tm,)),
            dma((tm,)),
            dma((tm,)),
            dma((tm + space,)),
            dma((tm + space,)),
        ],
        compiler_params=pltpu.CompilerParams(
            collective_id=0, has_side_effects=True, vmem_limit_bytes=48 * 1024 * 1024
        ),
    )(
        obs_rows[0], obs_weight, error_inverse, rates,
        checkpoint[0], advect[0], diffuse[0], obs_values[0],
    )
    entries = tm * space * checkpoint.size
    rms_value = jnp.sqrt(jnp.sum(sums) / entries + 1e-06)
    direction = back.reshape(checkpoint.shape) / rms_value
    return direction, rms_value


def solution(mesh):
    placed = (
        P("tm", None, "space", None),
        P("tm", None, "space", None),
        P("tm", "space", None),
        P("tm", None, "space"),
        P("tm", None, "space", None, None, None),
        P("tm"),
        P("tm", None),
        P(),
    )
    return jax.shard_map(
        functools.partial(on_device, mesh.shape["tm"], mesh.shape["space"]),
        mesh=mesh,
        in_specs=placed,
        out_specs=(P("tm", None, "space", None), P()),
        check_vma=False,
    )
```

```python
import functools

import jax
import jax.numpy as jnp
from jax import lax
from jax.experimental import pallas as pl
from jax.experimental.pallas import tpu as pltpu
from jax.sharding import PartitionSpec as P

MESH = pl.DeviceIdType.MESH
LANES = 128


def kernel(
    tm,
    space,
    rows_hbm,
    weight_hbm,
    einv_hbm,
    rates_hbm,
    ck_hbm,
    adv_hbm,
    dif_hbm,
    obs_hbm,
    back_ref,
    rms_ref,
    rows_smem,
    weight_smem,
    einv_smem,
    rates_smem,
    states,
    adv,
    dif,
    coef,
    obs,
    pull,
    count,
    next_ck,
    next_einv,
    prior_end,
    costate,
    grads,
    gathered,
    scanned,
    returned,
    part,
    part_tm,
    part_space,
    local_sem,
    halo_send,
    halo_recv,
    ck_send,
    ck_recv,
    pull_send,
    pull_recv,
    edge_send,
    edge_recv,
    end_send,
    end_recv,
    a2a_send,
    a2a_recv,
    ret_send,
    ret_recv,
    sum_send,
    sum_recv,
):
    comps, rows, cols = ck_hbm.shape
    steps, kobs, _, block, _ = obs_hbm.shape
    halo = 2 * steps
    wide = rows + 2 * halo
    tiles = rows // block
    tall, across_cols = grads.shape[2:]
    col_groups = cols // across_cols
    me = lax.axis_index("tm")
    sp = lax.axis_index("space")
    own = pl.ds(halo, rows)
    low_halo = pl.ds(0, halo)
    high_halo = pl.ds(halo + rows, halo)
    copies = []

    def send(src, dst, ssem, rsem, target, guard=None):
        copy = pltpu.make_async_remote_copy(
            src_ref=src, dst_ref=dst, send_sem=ssem, recv_sem=rsem,
            device_id=target, device_id_type=MESH,
        )
        if guard is None:
            copy.start()
        else:
            pl.when(guard)(copy.start)
        copies.append((copy, guard))
        return copy

    def landed(copy, guard=None):
        if guard is None:
            copy.wait_recv()
        else:
            pl.when(guard)(copy.wait_recv)

    has_north = sp < space - 1
    has_south = sp > 0
    north = {"space": jnp.minimum(sp + 1, space - 1)}
    south = {"space": jnp.maximum(sp - 1, 0)}
    has_next = me < tm - 1
    has_prev = me > 0
    nxt = {"tm": jnp.minimum(me + 1, tm - 1)}
    prv = {"tm": jnp.maximum(me - 1, 0)}

    barrier = pltpu.get_barrier_semaphore()
    for o in range(1, tm):
        pl.semaphore_signal(
            barrier, inc=1, device_id={"tm": lax.rem(me + o, tm)}, device_id_type=MESH
        )
    for o in range(1, space):
        pl.semaphore_signal(
            barrier, inc=1, device_id={"space": lax.rem(sp + o, space)}, device_id_type=MESH
        )

    loads = [
        pltpu.make_async_copy(source, target, local_sem.at[k])
        for k, (source, target) in enumerate(
            (
                (dif_hbm, dif.at[own]),
                (adv_hbm, adv.at[:, own]),
                (ck_hbm, states.at[0, :, own]),
                (rows_hbm, rows_smem),
                (weight_hbm, weight_smem),
                (einv_hbm, einv_smem),
                (rates_hbm, rates_smem),
                (obs_hbm, obs),
            )
        )
    ]
    for load in loads:
        load.start()

    @pl.when(jnp.logical_not(has_south))
    def _():
        states[0, :, 0:halo, :] = jnp.zeros((comps, halo, cols), jnp.float32)
        adv[:, 0:halo, :] = jnp.zeros((2, halo, cols), jnp.float32)
        dif[0:halo, :] = jnp.zeros((halo, cols), jnp.float32)
        pull[:, :, 0:block, :] = jnp.zeros((comps, steps, block, cols), jnp.float32)
        count[:, 0] = jnp.zeros((steps, block, LANES), jnp.float32)

    @pl.when(jnp.logical_not(has_north))
    def _():
        states[0, :, halo + rows : wide, :] = jnp.zeros((comps, halo, cols), jnp.float32)
        adv[:, halo + rows : wide, :] = jnp.zeros((2, halo, cols), jnp.float32)
        dif[halo + rows : wide, :] = jnp.zeros((halo, cols), jnp.float32)
        pull[:, :, block + rows :, :] = jnp.zeros((comps, steps, block, cols), jnp.float32)
        count[:, tiles + 1] = jnp.zeros((steps, block, LANES), jnp.float32)

    @pl.when(jnp.logical_not(has_next))
    def _():
        next_ck[...] = jnp.zeros_like(next_ck)
        next_einv[...] = jnp.zeros_like(next_einv)

    @pl.when(jnp.logical_not(has_prev))
    def _():
        prior_end[...] = jnp.zeros_like(prior_end)

    middle = steps // 2
    near = min(middle, block)
    if near < block:
        blank = jnp.zeros((comps, middle, block - near, cols), jnp.float32)
        pull[:, 0:middle, 0 : block - near, :] = blank
        pull[:, 0:middle, block + rows + near :, :] = blank

    for load in loads[:3]:
        load.wait()
    pl.semaphore_wait(barrier, tm + space - 2)

    def both_ways(ref, ssem, rsem):
        lead = (slice(None),) * (len(ref.shape) - 2)
        source = ref.at[lead + (own,)]
        return (
            send(source, ref.at[lead + (low_halo,)], ssem.at[0], rsem.at[0], north, has_north),
            send(source, ref.at[lead + (high_halo,)], ssem.at[1], rsem.at[1], south, has_south),
        )

    def both_landed(pair):
        landed(pair[0], has_south)
        landed(pair[1], has_north)

    def send_ck_halo(c):
        return both_ways(states.at[0, c], ck_send.at[c], ck_recv.at[c])

    halos = [
        both_ways(dif, halo_send.at[0], halo_recv.at[0]),
        both_ways(adv, halo_send.at[1], halo_recv.at[1]),
    ]
    ck_halos = [send_ck_halo(0)]
    next_copies = [
        send(states.at[0, c, own], next_ck.at[c], edge_send.at[c], edge_recv.at[c], prv, has_prev)
        for c in range(comps)
    ]

    for load in loads[3:7]:
        load.wait()
    weight = weight_smem[0]
    for c in range(comps):
        part[1, c : c + 1, :] = jnp.full((1, LANES), einv_smem[0, c], jnp.float32)

    @pl.loop(0, steps)
    def _(t):
        for b in range(tiles):
            total = jnp.float32(0.0)
            for i in range(kobs):
                total = total + jnp.where(rows_smem[i, t] == b, weight, 0.0)
            count[t, b + 1] = jnp.full((block, LANES), total, jnp.float32)

    einv_copy = send(part.at[1], next_einv, edge_send.at[comps], edge_recv.at[comps], prv, has_prev)
    count_copies = (
        send(count.at[:, tiles], count.at[:, 0], halo_send.at[2, 0], halo_recv.at[2, 0], north, has_north),
        send(count.at[:, 1], count.at[:, tiles + 1], halo_send.at[2, 1], halo_recv.at[2, 1], south, has_south),
    )
    loads[7].wait()

    @pl.loop(0, steps)
    def _(t):
        for b in range(tiles):
            picks = [jnp.where(rows_smem[i, t] == b, weight, 0.0) for i in range(kobs)]
            for c in range(comps):
                total = picks[0] * obs[t, 0, c]
                for i in range(1, kobs):
                    total = total + picks[i] * obs[t, i, c]
                pull[c, t, block * (b + 1) : block * (b + 2), :] = total

    spans = ((middle, steps - 1, block), (0, middle, near), (steps - 1, steps, block))

    def send_pull(c, which):
        first, last, depth = spans[which]
        at = pl.ds(first, last - first)
        return (
            send(
                pull.at[c, at, pl.ds(block + rows - depth, depth)],
                pull.at[c, at, pl.ds(block - depth, depth)],
                pull_send.at[c, which, 0], pull_recv.at[c, which, 0], north, has_north,
            ),
            send(
                pull.at[c, at, pl.ds(block, depth)],
                pull.at[c, at, pl.ds(block + rows, depth)],
                pull_send.at[c, which, 1], pull_recv.at[c, which, 1], south, has_south,
            ),
        )

    pulls = {}

    def send_pulls(c):
        pulls[c] = [send_pull(c, 0), send_pull(c, 1)]

    def next_row(c):
        return jnp.concatenate([next_einv[c : c + 1, :]] * (cols // LANES), axis=1)

    def send_last_pull(c):
        landed(next_copies[c], has_next)
        if c == 0:
            landed(einv_copy, has_next)
        inside = slice(block, block + rows)
        pull[c, steps - 1, inside, :] = pull[c, steps - 1, inside, :] + next_row(c) * next_ck[c]
        pulls[c].append(send_pull(c, 2))

    send_pulls(0)
    ck_halos.append(send_ck_halo(1))
    send_pulls(1)

    both_landed(halos[0])
    both_landed(halos[1])
    for r in range(0, wide, 8):
        at = slice(r, r + 8)
        d, a0, a1 = dif[at], adv[0, at], adv[1, at]
        coef[0, at] = 1.0 - 4.0 * d
        coef[1, at] = d - 0.5 * a0
        coef[2, at] = d + 0.5 * a0
        coef[3, at] = d - 0.5 * a1
        coef[4, at] = d + 0.5 * a1
    send_last_pull(0)

    end_copies = {}

    def forward(c):
        both_landed(ck_halos[c])

        @pl.loop(0, steps)
        def _(t):
            v = states[t, c]
            states[t + 1, c] = (
                coef[0] * v
                + coef[1] * pltpu.roll(v, cols - 1, 1)
                + coef[2] * pltpu.roll(v, 1, 1)
                + coef[3] * pltpu.roll(v, wide - 1, 0)
                + coef[4] * pltpu.roll(v, 1, 0)
            )

        end_copies[c] = send(
            states.at[steps, c, own], prior_end.at[c], end_send.at[c], end_recv.at[c], nxt, has_next
        )

    inner_rows = rows + 2 * block
    first = halo - block
    inner = pl.ds(first, inner_rows)
    gather = {}

    def adjoint(c, squares):
        for pair in pulls[c]:
            both_landed(pair)

        def force(t):
            marks = [
                jnp.concatenate([count[t, q]] * (cols // LANES), axis=1) for q in range(tiles + 2)
            ]
            return jnp.concatenate(marks, axis=0) * states[t + 1, c, inner] - pull[c, t]

        costate[...] = force(steps - 1) + next_row(c) * states[steps, c, inner]

        def step(w):
            return (
                coef[0, inner] * w
                + pltpu.roll(coef[1, inner] * w, 1, 1)
                + pltpu.roll(coef[2, inner] * w, cols - 1, 1)
                + pltpu.roll(coef[3, inner] * w, 1, 0)
                + pltpu.roll(coef[4, inner] * w, inner_rows - 1, 0)
            )

        @pl.loop(0, steps - 1)
        def _(s):
            costate[...] = step(costate[...]) + force(steps - 2 - s)

        landed(end_copies[c], has_prev)
        g = step(costate[...])[block : block + rows] + einv_smem[0, c] * (
            states[0, c, own] - prior_end[c]
        )
        for d in range(tm):
            r0, c0 = d // col_groups * tall, d % col_groups * across_cols
            grads[c, d] = g[r0 : r0 + tall, c0 : c0 + across_cols]
        gather[c] = [
            send(
                grads.at[c, lax.rem(me + o, tm)], gathered.at[c, me],
                a2a_send.at[c, o], a2a_recv.at[c, o], {"tm": lax.rem(me + o, tm)},
            )
            for o in range(1, tm)
        ]
        gathered[c, me] = grads[c, me]
        sq = g * g
        for r in range(0, rows, 8):
            for l in range(0, cols, LANES):
                squares = squares + sq[r : r + 8, l : l + LANES]
        return squares

    returns = {}

    def scan(c):
        for copy in gather[c]:
            copy.wait_recv()
        keep = [jnp.full((1, across_cols), rates_smem[c, j], jnp.float32) for j in range(tm)]
        gain = [jnp.sqrt(1.0 - r * r) for r in keep]
        running = jnp.zeros((tall, across_cols), jnp.float32)
        ahead = []
        for j in range(tm):
            running = keep[j] * running + gain[j] * gathered[c, j]
            ahead.append(running)
        running = jnp.zeros((tall, across_cols), jnp.float32)
        for j in range(tm - 1, -1, -1):
            running = gain[j] * ahead[j] + running
            scanned[c, j] = running
            running = keep[j] * running
        returns[c] = [
            send(
                scanned.at[c, lax.rem(me + o, tm)], returned.at[c, me],
                ret_send.at[c, o], ret_recv.at[c, o], {"tm": lax.rem(me + o, tm)},
            )
            for o in range(1, tm)
        ]
        returned[c, me] = scanned[c, me]

    squares = jnp.zeros((8, LANES), jnp.float32)
    forward(0)
    send_last_pull(1)
    ck_halos.append(send_ck_halo(2))
    send_pulls(2)
    forward(1)
    send_last_pull(2)
    ck_halos.append(send_ck_halo(3))
    send_pulls(3)
    both_landed(count_copies)
    squares = adjoint(0, squares)
    send_last_pull(3)
    forward(2)
    forward(3)
    squares = adjoint(1, squares)
    scan(0)
    squares = adjoint(2, squares)
    scan(1)
    squares = adjoint(3, squares)

    part[0] = squares
    sums = [
        send(
            part.at[0], part_tm.at[me], sum_send.at[o], sum_recv.at[o], {"tm": lax.rem(me + o, tm)}
        )
        for o in range(1, tm)
    ]
    part_tm[me] = squares
    scan(2)
    scan(3)

    for copy in sums:
        copy.wait_recv()
    total = part_tm[0]
    for j in range(1, tm):
        total = total + part_tm[j]
    part_space[sp] = total
    part[2] = total
    across = [
        send(
            part.at[2], part_space.at[sp], sum_send.at[tm + o], sum_recv.at[tm + o],
            {"space": lax.rem(sp + o, space)},
        )
        for o in range(1, space)
    ]

    def place(c):
        for copy in returns[c]:
            copy.wait_recv()
        for d in range(tm):
            r0, c0 = d // col_groups * tall, d % col_groups * across_cols
            back_ref[c, r0 : r0 + tall, c0 : c0 + across_cols] = returned[c, d]

    for c in range(comps - 1):
        place(c)
    for copy in across:
        copy.wait_recv()
    total = part_space[0]
    for j in range(1, space):
        total = total + part_space[j]
    entries = tm * space * comps * rows * cols
    rms_ref[...] = jnp.sqrt(jnp.sum(total, axis=(0, 1), keepdims=True) / entries + 1e-06)
    place(comps - 1)
    for copy, guard in copies:
        if guard is None:
            copy.wait_send()
        else:
            pl.when(guard)(copy.wait_send)


def on_device(tm, space, checkpoint, advect, diffuse, obs_rows, obs_values, obs_weight, error_inverse, rates):
    comps, rows, cols = checkpoint.shape[1:]
    steps, kobs, _, block, _ = obs_values.shape[1:]
    halo = 2 * steps
    wide = rows + 2 * halo
    tiles = rows // block
    col_groups = min(tm, cols // LANES)
    chunk = (rows * col_groups // tm, cols // col_groups)
    f32 = jnp.float32
    hbm = pl.BlockSpec(memory_space=pltpu.HBM)
    vmem = pl.BlockSpec(memory_space=pltpu.VMEM)
    dma = pltpu.SemaphoreType.DMA
    back, rms = pl.pallas_call(
        functools.partial(kernel, tm, space),
        out_shape=(
            jax.ShapeDtypeStruct((comps, rows, cols), f32),
            jax.ShapeDtypeStruct((1, 1), f32),
        ),
        in_specs=[hbm] * 8,
        out_specs=(vmem, vmem),
        scratch_shapes=[
            pltpu.SMEM((kobs, steps), jnp.int32),
            pltpu.SMEM((1,), f32),
            pltpu.SMEM((1, comps), f32),
            pltpu.SMEM((comps, tm), f32),
            pltpu.VMEM((steps + 1, comps, wide, cols), f32),
            pltpu.VMEM((2, wide, cols), f32),
            pltpu.VMEM((wide, cols), f32),
            pltpu.VMEM((5, wide, cols), f32),
            pltpu.VMEM((steps, kobs, comps, block, cols), f32),
            pltpu.VMEM((comps, steps, rows + 2 * block, cols), f32),
            pltpu.VMEM((steps, tiles + 2, block, LANES), f32),
            pltpu.VMEM((comps, rows, cols), f32),
            pltpu.VMEM((8, LANES), f32),
            pltpu.VMEM((comps, rows, cols), f32),
            pltpu.VMEM((rows + 2 * block, cols), f32),
            pltpu.VMEM((comps, tm) + chunk, f32),
            pltpu.VMEM((comps, tm) + chunk, f32),
            pltpu.VMEM((comps, tm) + chunk, f32),
            pltpu.VMEM((comps, tm) + chunk, f32),
            pltpu.VMEM((3, 8, LANES), f32),
            pltpu.VMEM((tm, 8, LANES), f32),
            pltpu.VMEM((space, 8, LANES), f32),
            dma((8,)),
            dma((3, 2)),
            dma((3, 2)),
            dma((comps, 2)),
            dma((comps, 2)),
            dma((comps, 3, 2)),
            dma((comps, 3, 2)),
            dma((comps + 1,)),
            dma((comps + 1,)),
            dma((comps,)),
            dma((comps,)),
            dma((comps, tm)),
            dma((comps, tm)),
            dma((comps, tm)),
            dma((comps, tm)),
            dma((tm + space,)),
            dma((tm + space,)),
        ],
        compiler_params=pltpu.CompilerParams(
            collective_id=0, has_side_effects=True, vmem_limit_bytes=60 * 1024 * 1024
        ),
    )(
        obs_rows[0].T, obs_weight, error_inverse, rates.T,
        checkpoint[0], advect[0], diffuse[0], obs_values[0],
    )
    rms_value = rms.reshape(())
    direction = back[None] / rms_value
    return direction, rms_value


def solution(mesh):
    placed = (
        P("tm", None, "space", None),
        P("tm", None, "space", None),
        P("tm", "space", None),
        P("tm", None, "space"),
        P("tm", None, "space", None, None, None),
        P("tm"),
        P("tm", None),
        P(),
    )
    return jax.shard_map(
        functools.partial(on_device, mesh.shape["tm"], mesh.shape["space"]),
        mesh=mesh,
        in_specs=placed,
        out_specs=(P("tm", None, "space", None), P()),
        check_vma=False,
    )
```
